32 devices in a mesh: chain: 16 (over z, x, core), tok: 2 (over y).
Axes of the slice: x: 2, y: 2, z: 4, core: 2. Of those that a mesh axis runs over, the one named last changes fastest.
Arguments:
- queries: bfloat16 [65536, 128], P(('chain', 'tok')), may hold values from -6 to 6
- keys: bfloat16 [65536, 128], P(('chain', 'tok')), may hold values from -6 to 6
- values: bfloat16 [65536, 128], P(('chain', 'tok')), may hold values from -6 to 6
Outputs:
- attended: bfloat16 [65536, 128], P(('chain', 'tok'))
The draws below stay inside these ranges and needn't reach their ends.
All inputs are finite; a program needn't handle non-finite values.
Results may differ from the reference program's by a relative error of at most 0.0058.
Values may be sent and summed in bfloat16 or wider, within the bound.
A program may use at most 64 MiB of HBM per device.

```python
import math
import jax
import jax.numpy as jnp
import numpy as np
from jax import lax

HD = 64
HEADS = 2
F = 2080
GROUP = 4096
TOKENS = 65536
N_CHAIN = 16


def levels(key, shape, pieces, low, largest):
    factor_of, own = 1.0, jax.random.fold_in(key, 6)
    for dim, parts in pieces:
        draws = jnp.exp(jax.random.uniform(jax.random.fold_in(own, dim), (parts,), jnp.float32, low / len(pieces), largest / len(pieces)))
        factor_of = factor_of * jnp.repeat(draws, shape[dim] // parts).reshape([-1 if axis == dim else 1 for axis in range(len(shape))])
    return factor_of


def normal_values(own_key, dims, scale, reach, pieces=(), held_as=jnp.bfloat16):
    array = scale * jax.random.normal(own_key, dims, jnp.float32)
    if pieces:
        array = array * levels(own_key, dims, pieces, -0.22, 0.18)
    return jnp.clip(array, -reach, reach).astype(held_as)


def setup_inputs(seed: int = 0) -> dict:
    streams_of = jax.random.split(jax.random.key(seed), 4)
    return {
        "queries": normal_values(streams_of[0], (TOKENS, HEADS * HD), 1.0, 6.0, ((0, 32),)),
        "keys": normal_values(streams_of[1], (TOKENS, HEADS * HD), 1.0, 6.0, ((0, 32),)),
        "values": normal_values(streams_of[2], (TOKENS, HEADS * HD), 1.0, 6.0, ((0, 32),)),
    }


def tables(width):
    first, second = np.triu_indices(width)
    places = np.arange(width)[:, None]
    first_pick = (places == first[None, :]).astype(np.float32)
    second_pick = (places == second[None, :]).astype(np.float32)
    scaling = np.where(first < second, math.sqrt(2.0), 1.0).astype(np.float32)
    return (jnp.asarray(first_pick), jnp.asarray(second_pick), jnp.asarray(scaling))

def expand(vectors, first_pick, second_pick, scaling):
    wide = vectors.astype(jnp.float32)
    left = jnp.dot(wide, first_pick, precision=lax.Precision.HIGHEST)
    right = jnp.dot(wide, second_pick, precision=lax.Precision.HIGHEST)
    rounded = (left * right * scaling[None, :]).astype(jnp.bfloat16)
    return lax.optimization_barrier(rounded).astype(jnp.float32)

def reference(queries, keys, values):
    first_pick, second_pick, scaling = tables(HD)
    shaped_q = jnp.transpose(queries.reshape(N_CHAIN, GROUP, HEADS, HD), (0, 2, 1, 3))
    shaped_k = jnp.transpose(keys.reshape(N_CHAIN, GROUP, HEADS, HD), (0, 2, 1, 3))
    shaped_v = jnp.transpose(values.reshape(N_CHAIN, GROUP, HEADS, HD), (0, 2, 1, 3))

    def head_state(pair):
        key_rows, value_rows = pair
        feats = expand(key_rows, first_pick, second_pick, scaling)
        return jnp.dot(feats.T, value_rows.astype(jnp.float32), precision=lax.Precision.HIGHEST)

    def head_read(pair):
        query_rows, state = pair
        feats = expand(query_rows, first_pick, second_pick, scaling)
        return jnp.dot(feats, state.astype(jnp.float32), precision=lax.Precision.HIGHEST)

    def step(prefix, inputs):
        index, query_group, key_group, value_group = inputs
        total = lax.map(head_state, (key_group, value_group))
        inclusive = prefix + total
        rounded = inclusive.astype(jnp.bfloat16)
        read = lax.map(head_read, (query_group, rounded))
        count = (index + 1).astype(jnp.float32) * GROUP
        result = (read / (HD * jnp.sqrt(count))).astype(jnp.bfloat16)
        return (inclusive, result)
    start = jnp.zeros((HEADS, F, HD), jnp.float32)
    order = jnp.arange(N_CHAIN, dtype=jnp.int32)
    _, outputs = lax.scan(step, start, (order, shaped_q, shaped_k, shaped_v))
    return jnp.transpose(outputs, (0, 2, 1, 3)).reshape(TOKENS, HEADS * HD)
```

```python
import functools
import math

import jax
import jax.numpy as jnp
from jax import lax
from jax.experimental import pallas as pl
from jax.experimental.pallas import tpu as pltpu
from jax.sharding import PartitionSpec as P

HD = 64
HEADS = 2
WIDE = HEADS * HD
FAR = HD // 2 + 1
BLOCKS = HD // 4 + 1
MESH = pl.DeviceIdType.MESH
F32, BF16 = jnp.float32, jnp.bfloat16


def layout(n_chain, n_tok):
    inner = 1 << ((n_chain.bit_length() - 1) // 2)
    plane = inner * n_tok
    row_parts = min(8, plane)
    blk_parts = plane // row_parts
    units = -(-BLOCKS // blk_parts)
    count = min(3, units)
    cuts = [-(-units * c // count) for c in range(count + 1)]
    return inner, plane, row_parts, blk_parts, units, cuts


def pairs(low, high):
    return [tuple(range(b, min(b + 2, high))) for b in range(low, high, 2)]


def kernel(n_chain, n_tok, q_ref, k_ref, v_ref, o_ref, xx, zz, vt, qf, acc, tot, got, plane_sum,
           far_got, inc_send, inc, out_t, rs_send, rs_recv, z_send, z_recv, ag_send, ag_recv):
    inner, plane, row_parts, blk_parts, units, cuts = layout(n_chain, n_tok)
    outer = n_chain // inner
    rows = WIDE // row_parts
    tokens = q_ref.shape[0]
    tile = 256 if tokens % 256 == 0 else tokens
    tiles = tokens // tile
    chain, tok = lax.axis_index("chain"), lax.axis_index("tok")
    z, me = chain // inner, (chain % inner) * n_tok + tok
    lane = lax.broadcasted_iota(jnp.int32, (tile, WIDE), 1)
    left = lane < HD

    def in_plane(k):
        peer = (me + k) % plane
        return peer, (z * inner + peer // n_tok, peer % n_tok)

    def along(k):
        return (((z + k) % outer) * inner + chain % inner, tok)

    barrier = pltpu.get_barrier_semaphore()
    for k in range(1, plane):
        pl.semaphore_signal(barrier, inc=1, device_id=in_plane(k)[1], device_id_type=MESH)
    for k in range(1, outer):
        pl.semaphore_signal(barrier, inc=1, device_id=along(k), device_id_type=MESH)

    def prepare(ref):
        @pl.loop(0, tiles)
        def _(t):
            at = pl.ds(pl.multiple_of(t * tile, tile), tile)
            x = ref[at, :].astype(F32)
            other = pltpu.roll(x, HD, 1)
            for h in range(HEADS):
                both = jnp.where(left, x, other) if h == 0 else jnp.where(left, other, x)
                xx[h, at, :] = both
                zz[h, at, :] = jnp.where(left, both, pltpu.roll(both, FAR, 1))

    root2 = math.sqrt(2.0)

    def feats(h, b, at):
        x = xx[h, at, :]
        product = zz[h, at, :] * (x if b == 0 else pltpu.roll(x, b, 1))
        if b == 0:
            scale = jnp.where(left, 1.0, 0.0).astype(F32)
        elif b == 1:
            scale = jnp.where(left, root2, 1.0).astype(F32)
        else:
            scale = jnp.float32(root2)
        return (product * scale).astype(BF16)

    def joined(parts, axis=1):
        return parts[0] if len(parts) == 1 else jnp.concatenate(parts, axis=axis)

    def blocks_of(c):
        return cuts[c] * blk_parts, cuts[c + 1] * blk_parts

    def state(c):
        low, high = blocks_of(c)
        real = min(high, BLOCKS)
        acc[pl.ds(low, high - low)] = jnp.zeros((high - low, WIDE, WIDE), F32)

        @pl.loop(0, tiles)
        def _(t):
            at = pl.ds(pl.multiple_of(t * tile, tile), tile)
            for group in pairs(low, real):
                for h in range(HEADS):
                    part = jnp.dot(vt[pl.ds(h * HD, HD), at],
                                   joined([feats(h, b, at) for b in group]),
                                   preferred_element_type=F32)
                    for i, b in enumerate(group):
                        acc[b, pl.ds(h * HD, HD), :] += part[:, i * WIDE:(i + 1) * WIDE]

        tot[pl.ds(low, high - low)] = acc[pl.ds(low, high - low)].astype(BF16)

    def spot(c, who):
        low, _ = blocks_of(c)
        size = cuts[c + 1] - cuts[c]
        row = pl.multiple_of((who % row_parts) * rows, rows)
        return pl.ds(low + (who // row_parts) * size, size), pl.ds(row, rows)

    def span(c):
        return pl.ds(cuts[c], cuts[c + 1] - cuts[c])

    started = []

    def scatter(c):
        for k in range(1, plane):
            peer, device = in_plane(k)
            blk, row = spot(c, peer)
            copy = pltpu.make_async_remote_copy(
                src_ref=tot.at[blk, row, :], dst_ref=got.at[k, span(c)],
                send_sem=rs_send.at[c, k], recv_sem=rs_recv.at[c, k],
                device_id=device, device_id_type=MESH)
            copy.start()
            started.append(copy)
            rs_copies[c].append(copy)
        blk, row = spot(c, me)
        got[0, span(c)] = tot[blk, row, :]

    def piece(c, source):
        return got[(me + plane - source) % plane, span(c)].astype(F32)

    def spread(c):
        for copy in rs_copies[c]:
            copy.wait_recv()
        total = piece(c, 0)
        for source in range(1, plane):
            total = total + piece(c, source)
        plane_sum[span(c)] = total.astype(BF16)
        for k in range(1, outer):
            copy = pltpu.make_async_remote_copy(
                src_ref=plane_sum.at[span(c)], dst_ref=far_got.at[k, span(c)],
                send_sem=z_send.at[c, k], recv_sem=z_recv.at[c, k],
                device_id=along(k), device_id_type=MESH)
            copy.start()
            started.append(copy)
            z_copies[c].append(copy)

    def gather(c):
        running = jnp.zeros((cuts[c + 1] - cuts[c], rows, WIDE), F32)
        for k in range(1, outer):
            z_copies[c][k - 1].wait_recv()
            running = running + jnp.where(k <= z, far_got[k, span(c)].astype(F32), 0.0)
        for g in range(inner):
            for y in range(n_tok):
                running = running + piece(c, g * n_tok + y)
            inc_send[g, span(c)] = running.astype(BF16)
        blk, row = spot(c, me)
        for k in range(1, plane):
            peer, device = in_plane(k)
            copy = pltpu.make_async_remote_copy(
                src_ref=inc_send.at[peer // n_tok, span(c)], dst_ref=inc.at[blk, row, :],
                send_sem=ag_send.at[c, k], recv_sem=ag_recv.at[c, k],
                device_id=device, device_id_type=MESH)
            copy.start()
            started.append(copy)
            ag_copies[c].append(copy)
        inc[blk, row, :] = inc_send[chain % inner, span(c)]

    def expand_queries(c):
        low, high = blocks_of(c)

        @pl.loop(0, tiles)
        def _(t):
            at = pl.ds(pl.multiple_of(t * tile, tile), tile)
            for b in range(low, min(high, BLOCKS)):
                for h in range(HEADS):
                    qf[h, b, at, :] = feats(h, b, at)

    def read(c, first, last):
        for copy in ag_copies[c]:
            copy.wait_recv()
        low, high = blocks_of(c)
        groups = pairs(low, min(high, BLOCKS))
        count = (chain + 1).astype(F32) * (tokens * n_tok)
        factor = 1.0 / (HD * jnp.sqrt(jnp.full((tile, WIDE), count, F32)))

        @pl.loop(0, tiles)
        def _(t):
            at = pl.ds(pl.multiple_of(t * tile, tile), tile)
            sums = []
            for h in range(HEADS):
                row = pl.ds(h * HD, HD)
                part = None if first else out_t[row, at]
                for group in groups:
                    more = lax.dot_general(
                        joined([inc[b, row, :] for b in group]),
                        joined([qf[h, b, at, :] for b in group]),
                        (((1,), (1,)), ((), ())), preferred_element_type=F32)
                    part = more if part is None else part + more
                if last:
                    sums.append(part)
                else:
                    out_t[row, at] = part
            if last:
                whole = jnp.concatenate(sums, axis=0).T
                o_ref[at, :] = (whole * factor).astype(BF16)

    n = len(cuts) - 1
    rs_copies, z_copies, ag_copies = ([[] for _ in range(n)] for _ in range(3))

    prepare(k_ref)

    @pl.loop(0, tiles)
    def _(t):
        at = pl.ds(pl.multiple_of(t * tile, tile), tile)
        vt[:, at] = v_ref[at, :].astype(F32).T.astype(BF16)

    for c in range(n):
        state(c)
        if c == 0:
            pl.semaphore_wait(barrier, plane - 1 + outer - 1)
        scatter(c)
        if c >= 1:
            spread(c - 1)
    prepare(q_ref)
    for c in range(n):
        expand_queries(c)
        if c == 0:
            spread(n - 1)
        gather(c)
    for c in range(n):
        read(c, c == 0, c == n - 1)
    for copy in started:
        copy.wait_send()


def on_device(n_chain, n_tok, queries, keys, values):
    inner, plane, row_parts, blk_parts, units, cuts = layout(n_chain, n_tok)
    outer, n = n_chain // inner, len(cuts) - 1
    rows, tokens = WIDE // row_parts, queries.shape[0]
    blocks = units * blk_parts
    sems = pltpu.SemaphoreType.DMA
    return pl.pallas_call(
        functools.partial(kernel, n_chain, n_tok),
        out_shape=jax.ShapeDtypeStruct((tokens, WIDE), BF16),
        in_specs=[pl.BlockSpec(memory_space=pltpu.VMEM)] * 3,
        out_specs=pl.BlockSpec(memory_space=pltpu.VMEM),
        scratch_shapes=[
            pltpu.VMEM((HEADS, tokens, WIDE), F32),
            pltpu.VMEM((HEADS, tokens, WIDE), F32),
            pltpu.VMEM((WIDE, tokens), BF16),
            pltpu.VMEM((HEADS, BLOCKS, tokens, WIDE), BF16),
            pltpu.VMEM((blocks, WIDE, WIDE), F32),
            pltpu.VMEM((blocks, WIDE, WIDE), BF16),
            pltpu.VMEM((plane, units, rows, WIDE), BF16),
            pltpu.VMEM((units, rows, WIDE), BF16),
            pltpu.VMEM((max(outer, 1), units, rows, WIDE), BF16),
            pltpu.VMEM((inner, units, rows, WIDE), BF16),
            pltpu.VMEM((blocks, WIDE, WIDE), BF16),
            pltpu.VMEM((WIDE, tokens), F32),
            sems((n, plane)), sems((n, plane)),
            sems((n, max(outer, 1))), sems((n, max(outer, 1))),
            sems((n, plane)), sems((n, plane)),
        ],
        compiler_params=pltpu.CompilerParams(
            collective_id=0, has_side_effects=True, vmem_limit_bytes=60 * 1024 * 1024),
    )(queries, keys, values)


def solution(mesh):
    placed = P(("chain", "tok"), None)
    return jax.shard_map(
        functools.partial(on_device, mesh.shape["chain"], mesh.shape["tok"]),
        mesh=mesh, in_specs=(placed,) * 3, out_specs=placed, check_vma=False)
```
